32 devices in a mesh: ctx: 16 (over z, y, x), tp: 2 (over core).
Axes of the slice: x: 2, y: 2, z: 4, core: 2. Of those that a mesh axis runs over, the one named last changes fastest.
Arguments:
- hidden_states: bfloat16 [4096, 8192], P('ctx', 'tp'), may hold values from -6 to 6
- queries: bfloat16 [4096, 4096], P('ctx', 'tp')
- key_matrix: bfloat16 [8192, 1024], P('tp'), may hold values from -0.0625 to 0.0625
- value_matrix: bfloat16 [8192, 1024], P('tp'), may hold values from -0.0625 to 0.0625
- stretch_table: int32 [32], replicated, may hold values from 0 to 31, as said below
Outputs:
- attended: bfloat16 [4096, 4096], P('ctx', 'tp')
The draws below stay inside these ranges and needn't reach their ends.
Inputs may be any that keep to these rules, and one draw needn't show every extreme that they name: `stretch_table`: a permutation of 0 to 31 in which entries 2 i and 2 i + 1 are two stretches c and 31 - c.
All inputs are finite; a program needn't handle non-finite values.
Results may differ from the reference program's by a relative error of at most 0.007.
The reference program's roundings to bfloat16 on the way count: a program that leaves them out, or rounds other values in their place, can miss the bound.
Values may be sent and summed in bfloat16 or wider, within the bound.
A program may use at most 256 MiB of HBM per device.

```python
import jax
import jax.numpy as jnp
from jax import lax

MODEL_WIDTH = 8192
QUERY_HEADS = 32
KEY_VALUE_HEADS = 8
HEAD_SIZE = 128
STRETCH = 128
STRETCHES = 32
SEQUENCE_TOKENS = 4096


def draw_queries(key, part):
    value_rows = jax.random.normal(jax.random.fold_in(key, 11), (SEQUENCE_TOKENS, QUERY_HEADS * HEAD_SIZE), jnp.float32)
    value_rows = jnp.clip(value_rows, -6.0, 6.0)
    return value_rows.astype(jnp.bfloat16)


def draw_stretch_table(key, part):
    half = STRETCHES // 2
    order = jax.random.permutation(jax.random.fold_in(key, 21), half).astype(jnp.int32)
    flips = jax.random.randint(jax.random.fold_in(key, 22), (half,), 0, 2).astype(jnp.int32)
    first = jnp.where(flips == 1, STRETCHES - 1 - order, order)
    second = STRETCHES - 1 - first
    return jnp.stack([first, second], axis=1).reshape(STRETCHES).astype(jnp.int32)


def steps_of(own_key, extent, shards, low, top_value):
    gain = 1.0
    for axis_at, parts in shards:
        draws = jax.random.uniform(jax.random.fold_in(jax.random.fold_in(own_key, 6), axis_at), (parts,), jnp.float32, low / len(shards), top_value / len(shards))
        gain = gain * jnp.repeat(jnp.exp(draws), extent[axis_at] // parts).reshape((-1,) + (1,) * (len(extent) - 1 - axis_at))
    return gain


def centred(stream_key, extent, spread, reach, split=(), kind=jnp.bfloat16):
    entries = spread * jax.random.normal(stream_key, extent, jnp.float32)
    if split:
        entries = entries * steps_of(stream_key, extent, split, -0.22, 0.18)
    return jnp.clip(entries, -reach, reach).astype(kind)


def setup_inputs(seed: int = 0) -> dict:
    splits = jax.random.split(jax.random.key(seed), 6)
    return {
        "hidden_states": centred(splits[0], (SEQUENCE_TOKENS, MODEL_WIDTH), 1.0, 6.0, ((0, 16), (1, 2))),
        "queries": draw_queries(jax.random.fold_in(splits[5], 71), 0),
        "key_matrix": centred(splits[2], (MODEL_WIDTH, KEY_VALUE_HEADS * HEAD_SIZE), MODEL_WIDTH ** -0.5, 0.0625, ((0, 2),)),
        "value_matrix": centred(splits[3], (MODEL_WIDTH, KEY_VALUE_HEADS * HEAD_SIZE), MODEL_WIDTH ** -0.5, 0.0625, ((0, 2),)),
        "stretch_table": draw_stretch_table(jax.random.fold_in(splits[5], 71), 0),
    }


def reference(hidden_states, queries, key_matrix, value_matrix, stretch_table):
    key_rows = jnp.dot(hidden_states, key_matrix, preferred_element_type=jnp.float32).astype(jnp.bfloat16)
    value_rows = jnp.dot(hidden_states, value_matrix, preferred_element_type=jnp.float32).astype(jnp.bfloat16)
    offsets = jnp.arange(SEQUENCE_TOKENS, dtype=jnp.int32)
    position = (jnp.repeat(stretch_table.astype(jnp.int32), STRETCH) * STRETCH + offsets % STRETCH).astype(jnp.int32)
    key_tiles = key_rows.astype(jnp.float32).reshape(SEQUENCE_TOKENS, KEY_VALUE_HEADS, HEAD_SIZE)
    value_tiles = value_rows.astype(jnp.float32).reshape(SEQUENCE_TOKENS, KEY_VALUE_HEADS, HEAD_SIZE)
    group_ratio = QUERY_HEADS // KEY_VALUE_HEADS
    rows_per_block = 128 if SEQUENCE_TOKENS % 128 == 0 else SEQUENCE_TOKENS
    query_block_list = queries.reshape(SEQUENCE_TOKENS // rows_per_block, rows_per_block, KEY_VALUE_HEADS, group_ratio, HEAD_SIZE)
    query_places = position.reshape(SEQUENCE_TOKENS // rows_per_block, rows_per_block)
    scale = 1.0 / (HEAD_SIZE ** 0.5)

    def one_block(items):
        query_block, places = items
        score = jnp.einsum('tgrd,ngd->grtn', query_block.astype(jnp.float32), key_tiles) * scale
        visible = position[None, :] <= places[:, None]
        masked = jnp.where(visible, score, jnp.float32(-1e30))
        highest = jnp.max(masked, axis=-1, keepdims=True)
        weight = jnp.where(visible, jnp.exp(masked - highest), jnp.float32(0.0))
        total = jnp.sum(weight, axis=-1)
        rounded = lax.optimization_barrier(weight.astype(jnp.bfloat16)).astype(jnp.float32)
        output = jnp.einsum('grtn,ngd->grtd', rounded, value_tiles) / total[..., None]
        return output.transpose(2, 0, 1, 3).reshape(rows_per_block, QUERY_HEADS * HEAD_SIZE).astype(jnp.bfloat16)

    outputs = lax.map(one_block, (query_block_list, query_places))
    return outputs.reshape(SEQUENCE_TOKENS, QUERY_HEADS * HEAD_SIZE)
```

```python
import functools

import jax
import jax.numpy as jnp
from jax import lax
from jax.experimental import pallas as pl
from jax.experimental.pallas import tpu as pltpu
from jax.sharding import PartitionSpec as P

KEY_VALUE_HEADS = 8
HEAD_SIZE = 128
D = HEAD_SIZE
ROWS = 256
NEG = -1e30
LOG2E = 1.4426950408889634
MESH = pl.DeviceIdType.MESH


def kernel(
    G, R, NG, S,
    table, hid_hbm, q_hbm, wk_hbm, wv_hbm, out_hbm,
    hid, w, terms, part_recv, stage, kvg, kvo, q_buf, qs, acc, mx, ls, o_send,
    hid_sem, w_sem, part_ssem, part_rsem, a2a_ssem, kvg_sem, kvo_sem, pair_ssem, group_ssem, other_ssem,
    q_ssem, q_rsem, o_ssem, o_rsem,
):
    me = lax.axis_index("ctx")
    c = lax.axis_index("tp")
    j = me % G
    plane = (me // G) % 2
    block = me // (2 * G)
    home = c == plane
    steps = (NG - 1) * G
    qw = R * D

    def peer(r):
        return (j // 2 + r // 2) % 2 * 2 + (j + r) % 2

    def across(r):
        return ((block * 2 + c) * G + peer(r), plane)

    def fetch(n):
        head = (c if n >= G else 1 - c) * G + peer(n % G)
        col = pl.multiple_of(head * D, D)
        a = pltpu.make_async_copy(wk_hbm.at[:, pl.ds(col, D)], w.at[n, :, pl.ds(0, D)], w_sem.at[n, 0])
        b = pltpu.make_async_copy(wv_hbm.at[:, pl.ds(col, D)], w.at[n, :, pl.ds(D, D)], w_sem.at[n, 1])
        return a, b

    hid_copy = pltpu.make_async_copy(hid_hbm, hid, hid_sem)
    hid_copy.start()
    for n in range(2 * G):
        for copy in fetch(n):
            copy.start()

    barrier = pltpu.get_barrier_semaphore()
    pl.semaphore_signal(barrier, inc=1, device_id=(me, 1 - c), device_id_type=MESH)
    for r in range(G):
        pl.semaphore_signal(barrier, inc=1, device_id=across(r), device_id_type=MESH)
    for gi in range(NG - 1):
        there = ((block + gi + 1) % NG * 2 + plane) * G + j
        pl.semaphore_signal(barrier, inc=1, device_id=(there, c), device_id_type=MESH)

    def q_src(r, h):
        return q_hbm.at[pl.ds(h * S, S), pl.ds(pl.multiple_of(peer(r) * qw, qw), qw)]

    def q_copy(r, h):
        return pltpu.make_async_remote_copy(
            src_ref=q_src(r, h),
            dst_ref=q_buf.at[r, h],
            send_sem=q_ssem.at[r, h],
            recv_sem=q_rsem.at[r, h],
            device_id=across(r),
            device_id_type=MESH,
        )

    def q_start(r, h):
        if r:
            q_copy(r, h).start()
        else:
            @pl.when(jnp.logical_not(home))
            def _():
                q_copy(r, h).start()

    @pl.when(home)
    def _():
        for h in range(2):
            pltpu.make_async_copy(q_src(0, h), q_buf.at[0, h], q_rsem.at[0, h]).start()

    def part_copy(r):
        return pltpu.make_async_remote_copy(
            src_ref=terms.at[r],
            dst_ref=part_recv.at[r],
            send_sem=part_ssem.at[r],
            recv_sem=part_rsem.at[r],
            device_id=(me, 1 - c),
            device_id_type=MESH,
        )

    def near(k, r):
        return kvg.at[:, :, pl.ds(pl.multiple_of((k * G + r) * S, S), S)]

    def far(gi, r, k):
        return kvo.at[gi, r, :, :, pl.ds(pl.multiple_of(k * S, S), S)]

    def a2a_copy(r):
        return pltpu.make_async_remote_copy(
            src_ref=stage.at[r],
            dst_ref=near(plane, r),
            send_sem=a2a_ssem.at[r],
            recv_sem=kvg_sem.at[plane, r],
            device_id=across(r),
            device_id_type=MESH,
        )

    def near_wait(k, r):
        pltpu.make_async_copy(near(k, r), near(k, r), kvg_sem.at[k, r]).wait()

    def pair_copy(r):
        return pltpu.make_async_remote_copy(
            src_ref=near(c, r),
            dst_ref=near(c, r),
            send_sem=pair_ssem.at[r],
            recv_sem=kvg_sem.at[c, r],
            device_id=(me, 1 - c),
            device_id_type=MESH,
        )

    def group_copy(gi, r):
        there = ((block + gi + 1) % NG * 2 + plane) * G + j
        return pltpu.make_async_remote_copy(
            src_ref=near(c, r),
            dst_ref=far(NG - 2 - gi, r, c),
            send_sem=group_ssem.at[gi, r],
            recv_sem=kvo_sem.at[NG - 2 - gi, r, c],
            device_id=(there, c),
            device_id_type=MESH,
        )

    def far_wait(s, k):
        gi, r = s // G, s % G
        pltpu.make_async_copy(far(gi, r, k), far(gi, r, k), kvo_sem.at[gi, r, k]).wait()

    def other_copy(s):
        gi, r = s // G, s % G
        return pltpu.make_async_remote_copy(
            src_ref=far(gi, r, c),
            dst_ref=far(gi, r, c),
            send_sem=other_ssem.at[gi, r],
            recv_sem=kvo_sem.at[gi, r, c],
            device_id=(me, 1 - c),
            device_id_type=MESH,
        )

    def pass_on(s):
        far_wait(s, c)
        other_copy(s).start()

    hid_copy.wait()

    def project(n, _):
        for i in range(2):
            half = w.at[n, :, pl.ds(i * D, D)]
            pltpu.make_async_copy(half, half, w_sem.at[n, i]).wait()
        terms[n] = jnp.dot(hid[...], w[n], preferred_element_type=jnp.float32)
        return 0

    lax.fori_loop(0, 2 * G, project, 0)

    pl.semaphore_wait(barrier, 1 + G + NG - 1)
    for r in range(G):
        part_copy(r).start()
    early = ((1, 0), (2, 0))
    for r, h in early:
        q_start(r, h)

    flip = table[2 * me] > table[2 * me + 1]
    for r in range(G):
        part_copy(r).wait_recv()
        both = (terms[G + r] + part_recv[r]).astype(jnp.bfloat16)
        ends = []
        for i in range(2):
            first = both[0:S, i * D:(i + 1) * D]
            second = both[S:2 * S, i * D:(i + 1) * D]
            ends.append((jnp.where(flip, second, first), jnp.where(flip, first, second)))
        if r == 0:
            @pl.when(home)
            def _():
                for i in range(2):
                    for side in range(2):
                        kvg[i, side, pl.ds(pl.multiple_of(c * G * S, S), S)] = ends[i][side]
                pair_copy(0).start()
                for gi in range(NG - 1):
                    group_copy(gi, 0).start()

            @pl.when(jnp.logical_not(home))
            def _():
                for i in range(2):
                    for side in range(2):
                        stage[r, i, side] = ends[i][side]
                a2a_copy(0).start()
        else:
            for i in range(2):
                for side in range(2):
                    stage[r, i, side] = ends[i][side]
            a2a_copy(r).start()
    for r in range(G):
        for h in range(2):
            if (r, h) not in early:
                q_start(r, h)

    for r in range(G):
        def relay():
            near_wait(c, r)
            pair_copy(r).start()
            for gi in range(NG - 1):
                group_copy(gi, r).start()

        if r:
            relay()
        else:
            pl.when(jnp.logical_not(home))(relay)

    def ids(ctx):
        a = table[2 * ctx]
        b = table[2 * ctx + 1]
        return jnp.minimum(a, b), jnp.maximum(a, b)

    def q_ctx(r):
        return (block * 2 + c) * G + peer(r)

    def sort_queries(r):
        for h in range(2):
            q_copy(r, h).wait_recv()
        ctx = q_ctx(r)
        turned = table[2 * ctx] > table[2 * ctx + 1]
        first = q_buf[r, 0]
        second = q_buf[r, 1]
        low = jnp.where(turned, second, first)
        high = jnp.where(turned, first, second)
        for i in range(R):
            qs[r, 0, i * S:(i + 1) * S] = low[:, i * D:(i + 1) * D]
            qs[r, 1, i * S:(i + 1) * S] = high[:, i * D:(i + 1) * D]

    rows_all = R * S
    rows_at = min(ROWS, rows_all)
    scale2 = LOG2E / D**0.5

    def unit(keys, values, places, first, r, h, at):
        rows = pl.ds(pl.multiple_of(at * rows_at, rows_at), rows_at)
        qx = qs[r, h, rows]
        tq = ids(q_ctx(r))[h]
        if first:
            row = lax.broadcasted_iota(jnp.int32, (rows_at, S), 0) % S
            col = lax.broadcasted_iota(jnp.int32, (rows_at, S), 1)
            diff = col - row
        pieces = []
        for side in range(h + 1):
            s = lax.dot_general(
                qx, keys(side), (((1,), (1,)), ((), ())), preferred_element_type=jnp.float32
            )
            for n, place in enumerate(places):
                part = s[:, n * S:(n + 1) * S]
                if side == h:
                    tk = ids(place)[side]
                    if first:
                        part = jnp.where(diff <= (tq - tk) * S, part, jnp.float32(NEG))
                    else:
                        part = part + jnp.where(tk < tq, jnp.float32(0), jnp.float32(NEG))
                pieces.append(part)
        top = pieces[0]
        for part in pieces[1:]:
            top = jnp.maximum(top, part)
        top = jnp.max(top, axis=1, keepdims=True)
        if first:
            new = jnp.broadcast_to(top, (rows_at, D))
        else:
            old = mx[r, h, rows]
            new = jnp.maximum(old, top)
        shift = new * scale2
        weights = [jnp.exp2(part * scale2 - shift) for part in pieces]
        total = weights[0]
        for weight in weights[1:]:
            total = total + weight
        value = None
        count = len(places)
        for side in range(h + 1):
            weight = jnp.concatenate(
                [x.astype(jnp.bfloat16) for x in weights[side * count:(side + 1) * count]], axis=1
            )
            term = jnp.dot(weight, values(side), preferred_element_type=jnp.float32)
            value = term if value is None else value + term
        if first:
            acc[r, h, rows] = value
            ls[r, h, rows] = total
        else:
            factor = jnp.exp2(old * scale2 - shift)
            acc[r, h, rows] = acc[r, h, rows] * factor + value
            ls[r, h, rows] = ls[r, h, rows] * factor + total
        mx[r, h, rows] = new

    def visit_near(r):
        places = [(block * 2 + k) * G + peer(i) for k in range(2) for i in range(G)]

        def step(at, _):
            for h in range(2):
                unit(lambda side: kvg[0, side], lambda side: kvg[1, side], places, True, r, h, at)
            return 0

        lax.fori_loop(0, rows_all // rows_at, step, 0)

    def visit_far(s, r):
        gi, i = s // G, s % G
        places = [((block + gi + 1) % NG * 2 + k) * G + peer(i) for k in range(2)]

        def step(at, _):
            for h in range(2):
                unit(lambda side: kvo[gi, i, 0, side], lambda side: kvo[gi, i, 1, side], places, False, r, h, at)
            return 0

        lax.fori_loop(0, rows_all // rows_at, step, 0)

    for r in range(G):
        near_wait(1 - c, r)

    def near_step(r, _):
        sort_queries(r)
        visit_near(r)

        @pl.when(r < min(2, steps))
        def _():
            pass_on(r)

        return 0

    lax.fori_loop(0, G, near_step, 0)

    def far_step(s, _):
        far_wait(s, 1 - c)

        def one(r, _):
            visit_far(s, r)
            return 0

        lax.fori_loop(0, G, one, 0)

        @pl.when(s >= 1)
        def _():
            pass_on(s + 1)

        return 0

    lax.fori_loop(0, steps - 1, far_step, 0)

    def o_dst():
        return out_hbm.at[:, pl.ds(pl.multiple_of(j * qw, qw), qw)]

    def o_copy(r):
        return pltpu.make_async_remote_copy(
            src_ref=o_send.at[r],
            dst_ref=o_dst(),
            send_sem=o_ssem.at[r],
            recv_sem=o_rsem.at[r],
            device_id=across(r),
            device_id_type=MESH,
        )

    far_wait(steps - 1, 1 - c)

    def finish(i, _):
        r = G - 1 - i
        visit_far(steps - 1, r)
        ctx = q_ctx(r)
        turned = table[2 * ctx] > table[2 * ctx + 1]
        for i in range(R):
            rows = slice(i * S, (i + 1) * S)
            ends = [
                (acc[r, h, rows] / jnp.sum(ls[r, h, rows], axis=1, keepdims=True)).astype(jnp.bfloat16)
                for h in range(2)
            ]
            o_send[r, 0:S, i * D:(i + 1) * D] = jnp.where(turned, ends[1], ends[0])
            o_send[r, S:2 * S, i * D:(i + 1) * D] = jnp.where(turned, ends[0], ends[1])

        @pl.when(jnp.logical_or(r > 0, jnp.logical_not(home)))
        def _():
            o_copy(r).start()

        return 0

    lax.fori_loop(0, G, finish, 0)
    mine = pltpu.make_async_copy(o_send.at[0], o_dst(), o_rsem.at[0])

    @pl.when(home)
    def _():
        mine.start()

    for r in range(G):
        part_copy(r).wait_send()
        pair_copy(r).wait_send()
        for gi in range(NG - 1):
            group_copy(gi, r).wait_send()

        def sent():
            a2a_copy(r).wait_send()
            for h in range(2):
                q_copy(r, h).wait_send()
            o_copy(r).wait_send()

        if r:
            sent()
        else:
            pl.when(jnp.logical_not(home))(sent)
    for s in range(steps):
        other_copy(s).wait_send()
    for r in range(G):
        o_copy(r).wait_recv()


def body(hidden_states, queries, key_matrix, value_matrix, stretch_table):
    tokens, width = hidden_states.shape
    G = KEY_VALUE_HEADS // lax.axis_size("tp")
    NG = lax.axis_size("ctx") // (2 * G)
    S = tokens // 2
    R = queries.shape[1] // (G * D)
    any_ = pl.BlockSpec(memory_space=pl.ANY)
    bf, f32 = jnp.bfloat16, jnp.float32
    dma = pltpu.SemaphoreType.DMA
    return pl.pallas_call(
        functools.partial(kernel, G, R, NG, S),
        out_shape=jax.ShapeDtypeStruct(queries.shape, bf),
        in_specs=[pl.BlockSpec(memory_space=pltpu.SMEM)] + [any_] * 4,
        out_specs=any_,
        scratch_shapes=[
            pltpu.VMEM((tokens, width), bf),
            pltpu.VMEM((2 * G, width, 2 * D), bf),
            pltpu.VMEM((2 * G, tokens, 2 * D), f32),
            pltpu.VMEM((G, tokens, 2 * D), f32),
            pltpu.VMEM((G, 2, 2, S, D), bf),
            pltpu.VMEM((2, 2, 2 * G * S, D), bf),
            pltpu.VMEM((NG - 1, G, 2, 2, 2 * S, D), bf),
            pltpu.VMEM((G, 2, S, R * D), bf),
            pltpu.VMEM((G, 2, R * S, D), bf),
            pltpu.VMEM((G, 2, R * S, D), f32),
            pltpu.VMEM((G, 2, R * S, D), f32),
            pltpu.VMEM((G, 2, R * S, D), f32),
            pltpu.VMEM((G, tokens, R * D), bf),
            dma,
            dma((2 * G, 2)),
            dma((G,)),
            dma((G,)),
            dma((G,)),
            dma((2, G)),
            dma((NG - 1, G, 2)),
            dma((G,)),
            dma((NG - 1, G)),
            dma((NG - 1, G)),
            dma((G, 2)),
            dma((G, 2)),
            dma((G,)),
            dma((G,)),
        ],
        compiler_params=pltpu.CompilerParams(
            collective_id=0, has_side_effects=True, vmem_limit_bytes=60 * 1024 * 1024
        ),
        name="fused",
    )(stretch_table, hidden_states, queries, key_matrix, value_matrix)


def solution(mesh):
    in_specs = (P("ctx", "tp"), P("ctx", "tp"), P("tp", None), P("tp", None), P())
    out_specs = P("ctx", "tp")
    return jax.shard_map(body, mesh=mesh, in_specs=in_specs, out_specs=out_specs, check_vma=False)
```

```python
import functools

import jax
import jax.numpy as jnp
from jax import lax
from jax.experimental import pallas as pl
from jax.experimental.pallas import tpu as pltpu
from jax.sharding import PartitionSpec as P

KEY_VALUE_HEADS = 8
HEAD_SIZE = 128
D = HEAD_SIZE
ROWS = 128
NEG = -1e30
AHEAD = 3
BEFORE = 6
LOG2E = 1.4426950408889634
MESH = pl.DeviceIdType.MESH


def kernel(
    G, R, NG, S,
    table, hid_hbm, q_hbm, wk_hbm, wv_hbm, out_hbm,
    hid, w, terms, part_recv, stage, kvg, kvo, q_buf, qs, acc, mx, ls, sc0, tp0, sc1, tp1, o_send,
    hid_sem, w_sem, part_ssem, part_rsem, a2a_ssem, kvg_sem, kvo_sem, pair_ssem, group_ssem, direct_ssem, other_ssem,
    q_ssem, q_rsem, o_ssem, o_rsem,
):
    me = lax.axis_index("ctx")
    c = lax.axis_index("tp")
    j = me % G
    plane = (me // G) % 2
    block = me // (2 * G)
    home = c == plane
    halves = G // 2
    steps = (NG - 1) * G
    batches = (NG - 1) * halves
    qw = R * D

    def peer(r):
        return (j // 2 + r // 2) % 2 * 2 + (j + r) % 2

    def across(r):
        return ((block * 2 + c) * G + peer(r), plane)

    def fetch(n):
        head = (c + 1 + n // G) % 2 * G + peer(n % G)
        col = pl.multiple_of(head * D, D)
        a = pltpu.make_async_copy(wk_hbm.at[:, pl.ds(col, D)], w.at[n, :, pl.ds(0, D)], w_sem.at[n, 0])
        b = pltpu.make_async_copy(wv_hbm.at[:, pl.ds(col, D)], w.at[n, :, pl.ds(D, D)], w_sem.at[n, 1])
        return a, b

    hid_copy = pltpu.make_async_copy(hid_hbm, hid, hid_sem)
    hid_copy.start()
    for n in range(AHEAD):
        for copy in fetch(n):
            copy.start()

    barrier = pltpu.get_barrier_semaphore()
    pl.semaphore_signal(barrier, inc=1, device_id=(me, 1 - c), device_id_type=MESH)
    for r in range(G):
        pl.semaphore_signal(barrier, inc=1, device_id=across(r), device_id_type=MESH)
    for gi in range(NG - 1):
        there = ((block + gi + 1) % NG * 2 + plane) * G + j
        pl.semaphore_signal(barrier, inc=1, device_id=(there, c), device_id_type=MESH)
        for r in range(G):
            there = ((block + gi + 1) % NG * 2 + c) * G + peer(r)
            pl.semaphore_signal(barrier, inc=1, device_id=(there, plane), device_id_type=MESH)

    def q_src(r, h):
        return q_hbm.at[pl.ds(h * S, S), pl.ds(pl.multiple_of(peer(r) * qw, qw), qw)]

    def q_copy(r, h):
        return pltpu.make_async_remote_copy(
            src_ref=q_src(r, h),
            dst_ref=q_buf.at[r, h],
            send_sem=q_ssem.at[r, h],
            recv_sem=q_rsem.at[r, h],
            device_id=across(r),
            device_id_type=MESH,
        )

    def q_start(r, h):
        if r:
            q_copy(r, h).start()
        else:
            @pl.when(jnp.logical_not(home))
            def _():
                q_copy(r, h).start()

    @pl.when(home)
    def _():
        for h in range(2):
            pltpu.make_async_copy(q_src(0, h), q_buf.at[0, h], q_rsem.at[0, h]).start()

    def part_copy(r):
        return pltpu.make_async_remote_copy(
            src_ref=terms.at[r],
            dst_ref=part_recv.at[r],
            send_sem=part_ssem.at[r],
            recv_sem=part_rsem.at[r],
            device_id=(me, 1 - c),
            device_id_type=MESH,
        )

    def near(k, r):
        return kvg.at[:, :, pl.ds(pl.multiple_of((k * G + r) * S, S), S)]

    def far(gi, r, k):
        return kvo.at[gi, r // 2, :, :, pl.ds(pl.multiple_of((r % 2 * 2 + k) * S, S), S)]

    def a2a_copy(r):
        return pltpu.make_async_remote_copy(
            src_ref=stage.at[r],
            dst_ref=near(plane, r),
            send_sem=a2a_ssem.at[r],
            recv_sem=kvg_sem.at[plane, r],
            device_id=across(r),
            device_id_type=MESH,
        )

    def near_wait(k, r):
        pltpu.make_async_copy(near(k, r), near(k, r), kvg_sem.at[k, r]).wait()

    def pair_copy(r):
        return pltpu.make_async_remote_copy(
            src_ref=near(c, r),
            dst_ref=near(c, r),
            send_sem=pair_ssem.at[r],
            recv_sem=kvg_sem.at[c, r],
            device_id=(me, 1 - c),
            device_id_type=MESH,
        )

    def group_copy(gi, r):
        there = ((block + gi + 1) % NG * 2 + plane) * G + j
        return pltpu.make_async_remote_copy(
            src_ref=near(c, r),
            dst_ref=far(NG - 2 - gi, r, c),
            send_sem=group_ssem.at[gi, r],
            recv_sem=kvo_sem.at[NG - 2 - gi, r, c],
            device_id=(there, c),
            device_id_type=MESH,
        )

    def facing(gi, p):
        there = (block + gi + 1) % NG
        return jnp.where(there > block, p, 1 - p) == 1

    def direct_copy(gi, r):
        there = ((block + gi + 1) % NG * 2 + c) * G + peer(r)
        return pltpu.make_async_remote_copy(
            src_ref=stage.at[r],
            dst_ref=far(NG - 2 - gi, r, plane),
            send_sem=direct_ssem.at[gi, r],
            recv_sem=kvo_sem.at[NG - 2 - gi, r, plane],
            device_id=(there, plane),
            device_id_type=MESH,
        )

    def far_wait(s, k):
        gi, r = s // G, s % G
        pltpu.make_async_copy(far(gi, r, k), far(gi, r, k), kvo_sem.at[gi, r, k]).wait()

    def other_copy(s):
        gi, r = s // G, s % G
        return pltpu.make_async_remote_copy(
            src_ref=far(gi, r, c),
            dst_ref=far(gi, r, c),
            send_sem=other_ssem.at[gi, r],
            recv_sem=kvo_sem.at[gi, r, c],
            device_id=(me, 1 - c),
            device_id_type=MESH,
        )

    def pass_on(s):
        far_wait(s, c)
        other_copy(s).start()

    hid_copy.wait()

    def project(n, _):
        for i in range(2):
            half = w.at[n, :, pl.ds(i * D, D)]
            pltpu.make_async_copy(half, half, w_sem.at[n, i]).wait()

        @pl.when(n + AHEAD < 2 * G)
        def _():
            for copy in fetch(n + AHEAD):
                copy.start()

        terms[n] = jnp.dot(hid[...], w[n], preferred_element_type=jnp.float32)
        return 0

    lax.fori_loop(0, BEFORE, project, 0)

    pl.semaphore_wait(barrier, 1 + G + (NG - 1) * (1 + G))
    for r in range(G):
        part_copy(r).start()
    early = ((1, 0), (2, 0))
    for r, h in early:
        q_start(r, h)

    lax.fori_loop(BEFORE, 2 * G, project, 0)

    def direct(r):
        for gi in range(NG - 1):
            @pl.when(facing(gi, plane))
            def _():
                direct_copy(gi, r).start()

    flip = table[2 * me] > table[2 * me + 1]
    for r in range(G):
        part_copy(r).wait_recv()
        both = (terms[G + r] + part_recv[r]).astype(jnp.bfloat16)
        ends = []
        for i in range(2):
            first = both[0:S, i * D:(i + 1) * D]
            second = both[S:2 * S, i * D:(i + 1) * D]
            ends.append((jnp.where(flip, second, first), jnp.where(flip, first, second)))
        if r == 0:
            @pl.when(home)
            def _():
                for i in range(2):
                    for side in range(2):
                        kvg[i, side, pl.ds(pl.multiple_of(c * G * S, S), S)] = ends[i][side]
                pair_copy(0).start()
                for gi in range(NG - 1):
                    group_copy(gi, 0).start()

            @pl.when(jnp.logical_not(home))
            def _():
                for i in range(2):
                    for side in range(2):
                        stage[r, i, side] = ends[i][side]
                a2a_copy(0).start()
                direct(0)
        else:
            for i in range(2):
                for side in range(2):
                    stage[r, i, side] = ends[i][side]
            a2a_copy(r).start()
            pl.when(jnp.logical_not(home))(functools.partial(direct, r))
    for r in range(G):
        for h in range(2):
            if (r, h) not in early:
                q_start(r, h)

    for r in range(G):
        def relay():
            near_wait(c, r)
            pair_copy(r).start()
            for gi in range(NG - 1):
                @pl.when(jnp.logical_or(home, jnp.logical_not(facing(gi, c))))
                def _():
                    group_copy(gi, r).start()

        if r:
            relay()
        else:
            pl.when(jnp.logical_not(home))(relay)

    def ids(ctx):
        a = table[2 * ctx]
        b = table[2 * ctx + 1]
        return jnp.minimum(a, b), jnp.maximum(a, b)

    def q_ctx(r):
        return (block * 2 + c) * G + peer(r)

    def sort_queries(r):
        for h in range(2):
            q_copy(r, h).wait_recv()
        ctx = q_ctx(r)
        turned = table[2 * ctx] > table[2 * ctx + 1]
        first = q_buf[r, 0]
        second = q_buf[r, 1]
        low = jnp.where(turned, second, first)
        high = jnp.where(turned, first, second)
        for i in range(R):
            qs[r, 0, i * S:(i + 1) * S] = low[:, i * D:(i + 1) * D]
            qs[r, 1, i * S:(i + 1) * S] = high[:, i * D:(i + 1) * D]

    rows_all = R * S
    rows_at = min(ROWS, rows_all)
    scale2 = LOG2E / D**0.5

    def score(to, tops, keys, places, first, r, at):
        rows = pl.ds(at * rows_at, rows_at)
        if first:
            row = lax.broadcasted_iota(jnp.int32, (rows_at, S), 0) % S
            col = lax.broadcasted_iota(jnp.int32, (rows_at, S), 1)
            diff = col - row
        for h in range(2):
            qx = qs[r, h, rows]
            tq = ids(q_ctx(r))[h]
            top = None
            for side in range(h + 1):
                s = lax.dot_general(
                    qx, keys(side), (((1,), (1,)), ((), ())), preferred_element_type=jnp.float32
                )
                for n, place in enumerate(places):
                    part = s[:, n * S:(n + 1) * S]
                    if side == h:
                        tk = ids(place)[side]
                        if first:
                            part = jnp.where(diff <= (tq - tk) * S, part, jnp.float32(NEG))
                        else:
                            part = part + jnp.where(tk < tq, jnp.float32(0), jnp.float32(NEG))
                    to[h + side, :, n * S:(n + 1) * S] = part
                    top = part if top is None else jnp.maximum(top, part)
            tops[h] = jnp.broadcast_to(jnp.max(top, axis=1, keepdims=True), (rows_at, D))

    def absorb(scores, tops, values, count, first, r, at):
        rows = pl.ds(at * rows_at, rows_at)
        for h in range(2):
            new = tops[h]
            if not first:
                old = mx[r, h, rows]
                new = jnp.maximum(old, new)
            shift = new * scale2
            total = None
            value = None
            for side in range(h + 1):
                weights = []
                for n in range(count):
                    weight = jnp.exp2(scores[h + side, :, n * S:(n + 1) * S] * scale2 - shift)
                    total = weight if total is None else total + weight
                    weights.append(weight.astype(jnp.bfloat16))
                term = jnp.dot(
                    jnp.concatenate(weights, axis=1), values(side), preferred_element_type=jnp.float32
                )
                value = term if value is None else value + term
            if first:
                acc[r, h, rows] = value
                ls[r, h, rows] = total
            else:
                factor = jnp.exp2(old * scale2 - shift)
                acc[r, h, rows] = acc[r, h, rows] * factor + value
                ls[r, h, rows] = ls[r, h, rows] * factor + total
            mx[r, h, rows] = new

    ways = ((sc0, tp0), (sc1, tp1))
    blocks = rows_all // rows_at

    def near_score(r, at):
        places = [(block * 2 + k) * G + peer(i) for k in range(2) for i in range(G)]
        score(*ways[at % 2], lambda side: kvg[0, side], places, True, r, at)

    def near_absorb(r, at):
        absorb(*ways[at % 2], lambda side: kvg[1, side], 2 * G, True, r, at)

    def far_score(b, r, at):
        gi, i = b // halves, b % halves
        there = (block + gi + 1) % NG * 2
        places = [(there + k) * G + peer(2 * i + a) for a in range(2) for k in range(2)]
        score(*ways[at % 2], lambda side: kvo[gi, i, 0, side], places, False, r, at)

    def far_absorb(b, r, at):
        gi, i = b // halves, b % halves
        absorb(*ways[at % 2], lambda side: kvo[gi, i, 1, side], 4, False, r, at)

    def through(score_at, absorb_at, r, then):
        for at in range(blocks):
            if at + 1 < blocks:
                score_at(r, at + 1)
            else:
                score_at(then, 0)
            absorb_at(r, at)

    for r in range(G):
        near_wait(1 - c, r)

    sort_queries(0)
    near_score(0, 0)

    def near_step(r, _):
        then = (r + 1) % G

        @pl.when(r + 1 < G)
        def _():
            sort_queries(then)

        through(near_score, near_absorb, r, then)

        @pl.when(r < 2)
        def _():
            pass_on(r)

        return 0

    lax.fori_loop(0, G, near_step, 0)

    def far_step(b, _):
        for a in range(2):
            far_wait(2 * b + a, 1 - c)
        far_score(b, 0, 0)

        def one(r, _):
            through(functools.partial(far_score, b), functools.partial(far_absorb, b), r, (r + 1) % G)
            return 0

        lax.fori_loop(0, G, one, 0)
        for a in range(2):
            pass_on(2 * b + 2 + a)
        return 0

    lax.fori_loop(0, batches - 1, far_step, 0)

    def o_dst():
        return out_hbm.at[:, pl.ds(pl.multiple_of(j * qw, qw), qw)]

    def o_copy(r):
        return pltpu.make_async_remote_copy(
            src_ref=o_send.at[r],
            dst_ref=o_dst(),
            send_sem=o_ssem.at[r],
            recv_sem=o_rsem.at[r],
            device_id=across(r),
            device_id_type=MESH,
        )

    for a in range(2):
        far_wait(steps - 2 + a, 1 - c)
    last = batches - 1
    far_score(last, G - 1, 0)

    def finish(i, _):
        r = G - 1 - i
        through(functools.partial(far_score, last), functools.partial(far_absorb, last), r, (r + G - 1) % G)
        ctx = q_ctx(r)
        turned = table[2 * ctx] > table[2 * ctx + 1]
        for i in range(R):
            rows = slice(i * S, (i + 1) * S)
            ends = [
                (acc[r, h, rows] / jnp.sum(ls[r, h, rows], axis=1, keepdims=True)).astype(jnp.bfloat16)
                for h in range(2)
            ]
            o_send[r, 0:S, i * D:(i + 1) * D] = jnp.where(turned, ends[1], ends[0])
            o_send[r, S:2 * S, i * D:(i + 1) * D] = jnp.where(turned, ends[0], ends[1])

        @pl.when(jnp.logical_or(r > 0, jnp.logical_not(home)))
        def _():
            o_copy(r).start()

        return 0

    lax.fori_loop(0, G, finish, 0)
    mine = pltpu.make_async_copy(o_send.at[0], o_dst(), o_rsem.at[0])

    @pl.when(home)
    def _():
        mine.start()

    for r in range(G):
        part_copy(r).wait_send()
        pair_copy(r).wait_send()
        for gi in range(NG - 1):
            @pl.when(jnp.logical_or(home, jnp.logical_not(facing(gi, c))))
            def _():
                group_copy(gi, r).wait_send()

            @pl.when(jnp.logical_and(facing(gi, plane), jnp.logical_not(home)))
            def _():
                direct_copy(gi, r).wait_send()

        def sent():
            a2a_copy(r).wait_send()
            for h in range(2):
                q_copy(r, h).wait_send()
            o_copy(r).wait_send()

        if r:
            sent()
        else:
            pl.when(jnp.logical_not(home))(sent)
    for s in range(steps):
        other_copy(s).wait_send()
    for r in range(G):
        o_copy(r).wait_recv()


def body(hidden_states, queries, key_matrix, value_matrix, stretch_table):
    tokens, width = hidden_states.shape
    G = KEY_VALUE_HEADS // lax.axis_size("tp")
    NG = lax.axis_size("ctx") // (2 * G)
    S = tokens // 2
    R = queries.shape[1] // (G * D)
    rows_at = min(ROWS, R * S)
    any_ = pl.BlockSpec(memory_space=pl.ANY)
    bf, f32 = jnp.bfloat16, jnp.float32
    dma = pltpu.SemaphoreType.DMA
    return pl.pallas_call(
        functools.partial(kernel, G, R, NG, S),
        out_shape=jax.ShapeDtypeStruct(queries.shape, bf),
        in_specs=[pl.BlockSpec(memory_space=pltpu.SMEM)] + [any_] * 4,
        out_specs=any_,
        scratch_shapes=[
            pltpu.VMEM((tokens, width), bf),
            pltpu.VMEM((2 * G, width, 2 * D), bf),
            pltpu.VMEM((2 * G, tokens, 2 * D), f32),
            pltpu.VMEM((G, tokens, 2 * D), f32),
            pltpu.VMEM((G, 2, 2, S, D), bf),
            pltpu.VMEM((2, 2, 2 * G * S, D), bf),
            pltpu.VMEM((NG - 1, G // 2, 2, 2, 4 * S, D), bf),
            pltpu.VMEM((G, 2, S, R * D), bf),
            pltpu.VMEM((G, 2, R * S, D), bf),
            pltpu.VMEM((G, 2, R * S, D), f32),
            pltpu.VMEM((G, 2, R * S, D), f32),
            pltpu.VMEM((G, 2, R * S, D), f32),
            pltpu.VMEM((3, rows_at, 2 * G * S), f32),
            pltpu.VMEM((2, rows_at, D), f32),
            pltpu.VMEM((3, rows_at, 2 * G * S), f32),
            pltpu.VMEM((2, rows_at, D), f32),
            pltpu.VMEM((G, tokens, R * D), bf),
            dma,
            dma((2 * G, 2)),
            dma((G,)),
            dma((G,)),
            dma((G,)),
            dma((2, G)),
            dma((NG - 1, G, 2)),
            dma((G,)),
            dma((NG - 1, G)),
            dma((NG - 1, G)),
            dma((NG - 1, G)),
            dma((G, 2)),
            dma((G, 2)),
            dma((G,)),
            dma((G,)),
        ],
        compiler_params=pltpu.CompilerParams(
            collective_id=0, has_side_effects=True, vmem_limit_bytes=60 * 1024 * 1024
        ),
        name="fused",
    )(stretch_table, hidden_states, queries, key_matrix, value_matrix)


def solution(mesh):
    in_specs = (P("ctx", "tp"), P("ctx", "tp"), P("tp", None), P("tp", None), P())
    out_specs = P("ctx", "tp")
    return jax.shard_map(body, mesh=mesh, in_specs=in_specs, out_specs=out_specs, check_vma=False)
```

```python
import functools

import jax
import jax.numpy as jnp
from jax import lax
from jax.experimental import pallas as pl
from jax.experimental.pallas import tpu as pltpu
from jax.sharding import PartitionSpec as P

KEY_VALUE_HEADS = 8
HEAD_SIZE = 128
D = HEAD_SIZE
ROWS = 128
NEG = -1e30
AHEAD = 3
BEFORE = 4
LOG2E = 1.4426950408889634
MESH = pl.DeviceIdType.MESH


def kernel(
    G, R, NG, S,
    table, hid_hbm, q_hbm, wk_hbm, wv_hbm, out_hbm,
    hid, w, terms, part_recv, stage, kvg, kvo, q_buf, qs, acc, mx, ls, sc0, tp0, sc1, tp1, o_send,
    hid_sem, w_sem, part_ssem, part_rsem, a2a_ssem, kvg_sem, kvo_sem, pair_ssem, group_ssem, direct_ssem, other_ssem,
    q_ssem, q_rsem, o_ssem, o_rsem,
):
    me = lax.axis_index("ctx")
    c = lax.axis_index("tp")
    j = me % G
    plane = (me // G) % 2
    block = me // (2 * G)
    home = c == plane
    halves = G // 2
    steps = (NG - 1) * G
    batches = (NG - 1) * halves
    qw = R * D

    def peer(r):
        return (j // 2 + r // 2) % 2 * 2 + (j + r) % 2

    def across(r):
        return ((block * 2 + c) * G + peer(r), plane)

    def fetch(n):
        head = (c + 1 + n // G) % 2 * G + peer(n % G)
        col = pl.multiple_of(head * D, D)
        a = pltpu.make_async_copy(wk_hbm.at[:, pl.ds(col, D)], w.at[n, :, pl.ds(0, D)], w_sem.at[n, 0])
        b = pltpu.make_async_copy(wv_hbm.at[:, pl.ds(col, D)], w.at[n, :, pl.ds(D, D)], w_sem.at[n, 1])
        return a, b

    hid_copy = pltpu.make_async_copy(hid_hbm, hid, hid_sem)
    hid_copy.start()
    for n in range(AHEAD):
        for copy in fetch(n):
            copy.start()

    barrier = pltpu.get_barrier_semaphore()
    pl.semaphore_signal(barrier, inc=1, device_id=(me, 1 - c), device_id_type=MESH)
    for r in range(G):
        pl.semaphore_signal(barrier, inc=1, device_id=across(r), device_id_type=MESH)
    for gi in range(NG - 1):
        there = ((block + gi + 1) % NG * 2 + plane) * G + j
        pl.semaphore_signal(barrier, inc=1, device_id=(there, c), device_id_type=MESH)
        for r in range(G):
            there = ((block + gi + 1) % NG * 2 + c) * G + peer(r)
            pl.semaphore_signal(barrier, inc=1, device_id=(there, plane), device_id_type=MESH)

    def q_src(r, h):
        return q_hbm.at[pl.ds(h * S, S), pl.ds(pl.multiple_of(peer(r) * qw, qw), qw)]

    def q_copy(r, h):
        return pltpu.make_async_remote_copy(
            src_ref=q_src(r, h),
            dst_ref=q_buf.at[r, h],
            send_sem=q_ssem.at[r, h],
            recv_sem=q_rsem.at[r, h],
            device_id=across(r),
            device_id_type=MESH,
        )

    def q_start(r, h):
        if r:
            q_copy(r, h).start()
        else:
            @pl.when(jnp.logical_not(home))
            def _():
                q_copy(r, h).start()

    @pl.when(home)
    def _():
        for h in range(2):
            pltpu.make_async_copy(q_src(0, h), q_buf.at[0, h], q_rsem.at[0, h]).start()

    def part_copy(r):
        return pltpu.make_async_remote_copy(
            src_ref=terms.at[r],
            dst_ref=part_recv.at[r],
            send_sem=part_ssem.at[r],
            recv_sem=part_rsem.at[r],
            device_id=(me, 1 - c),
            device_id_type=MESH,
        )

    def near(k, r):
        return kvg.at[:, :, pl.ds(pl.multiple_of((k * G + r) * S, S), S)]

    def far(gi, r, k):
        return kvo.at[gi, r // 2, :, :, pl.ds(pl.multiple_of((r % 2 * 2 + k) * S, S), S)]

    def a2a_copy(r):
        return pltpu.make_async_remote_copy(
            src_ref=stage.at[r],
            dst_ref=near(plane, r),
            send_sem=a2a_ssem.at[r],
            recv_sem=kvg_sem.at[plane, r],
            device_id=across(r),
            device_id_type=MESH,
        )

    def near_wait(k, r):
        pltpu.make_async_copy(near(k, r), near(k, r), kvg_sem.at[k, r]).wait()

    def pair_copy(r):
        return pltpu.make_async_remote_copy(
            src_ref=near(c, r),
            dst_ref=near(c, r),
            send_sem=pair_ssem.at[r],
            recv_sem=kvg_sem.at[c, r],
            device_id=(me, 1 - c),
            device_id_type=MESH,
        )

    def group_copy(gi, r):
        there = ((block + gi + 1) % NG * 2 + plane) * G + j
        return pltpu.make_async_remote_copy(
            src_ref=near(c, r),
            dst_ref=far(NG - 2 - gi, r, c),
            send_sem=group_ssem.at[gi, r],
            recv_sem=kvo_sem.at[NG - 2 - gi, r, c],
            device_id=(there, c),
            device_id_type=MESH,
        )

    def facing(gi, p):
        there = (block + gi + 1) % NG
        return jnp.where(there > block, p, 1 - p) == 1

    def direct_copy(gi, r):
        there = ((block + gi + 1) % NG * 2 + c) * G + peer(r)
        return pltpu.make_async_remote_copy(
            src_ref=stage.at[r],
            dst_ref=far(NG - 2 - gi, r, plane),
            send_sem=direct_ssem.at[gi, r],
            recv_sem=kvo_sem.at[NG - 2 - gi, r, plane],
            device_id=(there, plane),
            device_id_type=MESH,
        )

    def far_wait(s, k):
        gi, r = s // G, s % G
        pltpu.make_async_copy(far(gi, r, k), far(gi, r, k), kvo_sem.at[gi, r, k]).wait()

    def other_copy(s):
        gi, r = s // G, s % G
        return pltpu.make_async_remote_copy(
            src_ref=far(gi, r, c),
            dst_ref=far(gi, r, c),
            send_sem=other_ssem.at[gi, r],
            recv_sem=kvo_sem.at[gi, r, c],
            device_id=(me, 1 - c),
            device_id_type=MESH,
        )

    def pass_on(s):
        far_wait(s, c)
        other_copy(s).start()

    hid_copy.wait()

    def project(n, _):
        for i in range(2):
            half = w.at[n, :, pl.ds(i * D, D)]
            pltpu.make_async_copy(half, half, w_sem.at[n, i]).wait()

        @pl.when(n + AHEAD < 2 * G)
        def _():
            for copy in fetch(n + AHEAD):
                copy.start()

        terms[n] = jnp.dot(hid[...], w[n], preferred_element_type=jnp.float32)
        return 0

    lax.fori_loop(0, BEFORE, project, 0)

    pl.semaphore_wait(barrier, 1 + G + (NG - 1) * (1 + G))
    for r in range(G):
        part_copy(r).start()
    early = ((0, 0), (0, 1), (1, 0), (1, 1))
    for r, h in early:
        q_start(r, h)

    lax.fori_loop(BEFORE, 2 * G, project, 0)

    def direct(r):
        for gi in range(NG - 1):
            @pl.when(facing(gi, plane))
            def _():
                direct_copy(gi, r).start()

    flip = table[2 * me] > table[2 * me + 1]
    for r in range(G):
        part_copy(r).wait_recv()
        both = (terms[G + r] + part_recv[r]).astype(jnp.bfloat16)
        ends = []
        for i in range(2):
            first = both[0:S, i * D:(i + 1) * D]
            second = both[S:2 * S, i * D:(i + 1) * D]
            ends.append((jnp.where(flip, second, first), jnp.where(flip, first, second)))
        if r == 0:
            @pl.when(home)
            def _():
                for i in range(2):
                    for side in range(2):
                        kvg[i, side, pl.ds(pl.multiple_of(c * G * S, S), S)] = ends[i][side]
                pair_copy(0).start()
                for gi in range(NG - 1):
                    group_copy(gi, 0).start()

            @pl.when(jnp.logical_not(home))
            def _():
                for i in range(2):
                    for side in range(2):
                        stage[r, i, side] = ends[i][side]
                a2a_copy(0).start()
                direct(0)
        else:
            for i in range(2):
                for side in range(2):
                    stage[r, i, side] = ends[i][side]
            a2a_copy(r).start()
            pl.when(jnp.logical_not(home))(functools.partial(direct, r))
    for r in range(G):
        for h in range(2):
            if (r, h) not in early:
                q_start(r, h)

    for r in range(G):
        def relay():
            near_wait(c, r)
            pair_copy(r).start()
            for gi in range(NG - 1):
                @pl.when(jnp.logical_or(home, jnp.logical_not(facing(gi, c))))
                def _():
                    group_copy(gi, r).start()

        if r:
            relay()
        else:
            pl.when(jnp.logical_not(home))(relay)

    def ids(ctx):
        a = table[2 * ctx]
        b = table[2 * ctx + 1]
        return jnp.minimum(a, b), jnp.maximum(a, b)

    def q_ctx(r):
        return (block * 2 + c) * G + peer(r)

    def sort_queries(r):
        for h in range(2):
            q_copy(r, h).wait_recv()
        ctx = q_ctx(r)
        turned = table[2 * ctx] > table[2 * ctx + 1]
        first = q_buf[r, 0]
        second = q_buf[r, 1]
        low = jnp.where(turned, second, first)
        high = jnp.where(turned, first, second)
        for i in range(R):
            qs[r, 0, i * S:(i + 1) * S] = low[:, i * D:(i + 1) * D]
            qs[r, 1, i * S:(i + 1) * S] = high[:, i * D:(i + 1) * D]

    rows_all = R * S
    rows_at = min(ROWS, rows_all)
    scale2 = LOG2E / D**0.5

    def score(to, tops, keys, places, first, r, at):
        rows = pl.ds(at * rows_at, rows_at)
        if first:
            row = lax.broadcasted_iota(jnp.int32, (rows_at, S), 0) % S
            col = lax.broadcasted_iota(jnp.int32, (rows_at, S), 1)
            diff = col - row
        for h in range(2):
            qx = qs[r, h, rows]
            tq = ids(q_ctx(r))[h]
            top = None
            for side in range(h + 1):
                s = lax.dot_general(
                    qx, keys(side), (((1,), (1,)), ((), ())), preferred_element_type=jnp.float32
                )
                for n, place in enumerate(places):
                    part = s[:, n * S:(n + 1) * S]
                    if side == h:
                        tk = ids(place)[side]
                        if first:
                            part = jnp.where(diff <= (tq - tk) * S, part, jnp.float32(NEG))
                        else:
                            part = part + jnp.where(tk < tq, jnp.float32(0), jnp.float32(NEG))
                    to[h + side, :, n * S:(n + 1) * S] = part
                    top = part if top is None else jnp.maximum(top, part)
            tops[h] = jnp.broadcast_to(jnp.max(top, axis=1, keepdims=True), (rows_at, D))

    def absorb(scores, tops, values, count, first, r, at):
        rows = pl.ds(at * rows_at, rows_at)
        for h in range(2):
            new = tops[h]
            if not first:
                old = mx[r, h, rows]
                new = jnp.maximum(old, new)
            shift = new * scale2
            total = None
            value = None
            for side in range(h + 1):
                weights = []
                for n in range(count):
                    weight = jnp.exp2(scores[h + side, :, n * S:(n + 1) * S] * scale2 - shift)
                    total = weight if total is None else total + weight
                    weights.append(weight.astype(jnp.bfloat16))
                term = jnp.dot(
                    jnp.concatenate(weights, axis=1), values(side), preferred_element_type=jnp.float32
                )
                value = term if value is None else value + term
            if first:
                acc[r, h, rows] = value
                ls[r, h, rows] = total
            else:
                factor = jnp.exp2(old * scale2 - shift)
                acc[r, h, rows] = acc[r, h, rows] * factor + value
                ls[r, h, rows] = ls[r, h, rows] * factor + total
            mx[r, h, rows] = new

    ways = ((sc0, tp0), (sc1, tp1))
    blocks = rows_all // rows_at

    def near_score(k, own, r, at):
        places = [(block * 2 + k) * G + peer(i) for i in range(G)]
        at_k = pl.ds(pl.multiple_of(k * G * S, G * S), G * S)
        score(*ways[at % 2], lambda side: kvg[0, side, at_k], places, own, r, at)

    def near_absorb(k, own, r, at):
        at_k = pl.ds(pl.multiple_of(k * G * S, G * S), G * S)
        absorb(*ways[at % 2], lambda side: kvg[1, side, at_k], G, own, r, at)

    def far_score(b, r, at):
        gi, i = b // halves, b % halves
        there = (block + gi + 1) % NG * 2
        places = [(there + k) * G + peer(2 * i + a) for a in range(2) for k in range(2)]
        score(*ways[at % 2], lambda side: kvo[gi, i, 0, side], places, False, r, at)

    def far_absorb(b, r, at):
        gi, i = b // halves, b % halves
        absorb(*ways[at % 2], lambda side: kvo[gi, i, 1, side], 4, False, r, at)

    def through(score_at, absorb_at, r, then):
        for at in range(blocks):
            if at + 1 < blocks:
                score_at(r, at + 1)
            else:
                then()
            absorb_at(r, at)

    sort_queries(0)
    near_score(c, True, 0, 0)

    def near_step(r, _):
        after = (r + 1) % G

        @pl.when(r + 1 < G)
        def _():
            sort_queries(after)

        for at in range(blocks - 1):
            near_score(c, True, r, at + 1)
            near_absorb(c, True, r, at)

        @pl.when(r == 0)
        def _():
            for i in range(G):
                near_wait(1 - c, i)

        near_score(1 - c, False, r, 0)
        near_absorb(c, True, r, blocks - 1)
        through(
            functools.partial(near_score, 1 - c, False),
            functools.partial(near_absorb, 1 - c, False),
            r,
            functools.partial(near_score, c, True, after, 0),
        )

        @pl.when(r < 2)
        def _():
            pass_on(r)

        return 0

    lax.fori_loop(0, G, near_step, 0)
    pass_on(2)

    def far_step(b, _):
        for a in range(2):
            far_wait(2 * b + a, 1 - c)
        far_score(b, 0, 0)

        def one(r, _):
            through(
                functools.partial(far_score, b),
                functools.partial(far_absorb, b),
                r,
                functools.partial(far_score, b, (r + 1) % G, 0),
            )

            @pl.when(r == 2)
            def _():
                pass_on(2 * b + 3)

            return 0

        lax.fori_loop(0, G, one, 0)

        @pl.when(2 * b + 4 < steps)
        def _():
            pass_on(2 * b + 4)

        return 0

    lax.fori_loop(0, batches - 1, far_step, 0)

    def o_dst():
        return out_hbm.at[:, pl.ds(pl.multiple_of(j * qw, qw), qw)]

    def o_copy(r):
        return pltpu.make_async_remote_copy(
            src_ref=o_send.at[r],
            dst_ref=o_dst(),
            send_sem=o_ssem.at[r],
            recv_sem=o_rsem.at[r],
            device_id=across(r),
            device_id_type=MESH,
        )

    for a in range(2):
        far_wait(steps - 2 + a, 1 - c)
    last = batches - 1
    far_score(last, G - 1, 0)

    def finish(i, _):
        r = G - 1 - i
        through(
            functools.partial(far_score, last),
            functools.partial(far_absorb, last),
            r,
            functools.partial(far_score, last, (r + G - 1) % G, 0),
        )
        ctx = q_ctx(r)
        turned = table[2 * ctx] > table[2 * ctx + 1]
        for i in range(R):
            rows = slice(i * S, (i + 1) * S)
            ends = [
                (acc[r, h, rows] / jnp.sum(ls[r, h, rows], axis=1, keepdims=True)).astype(jnp.bfloat16)
                for h in range(2)
            ]
            o_send[r, 0:S, i * D:(i + 1) * D] = jnp.where(turned, ends[1], ends[0])
            o_send[r, S:2 * S, i * D:(i + 1) * D] = jnp.where(turned, ends[0], ends[1])

        @pl.when(jnp.logical_or(r > 0, jnp.logical_not(home)))
        def _():
            o_copy(r).start()

        return 0

    lax.fori_loop(0, G, finish, 0)
    mine = pltpu.make_async_copy(o_send.at[0], o_dst(), o_rsem.at[0])

    @pl.when(home)
    def _():
        mine.start()

    for r in range(G):
        part_copy(r).wait_send()
        pair_copy(r).wait_send()
        for gi in range(NG - 1):
            @pl.when(jnp.logical_or(home, jnp.logical_not(facing(gi, c))))
            def _():
                group_copy(gi, r).wait_send()

            @pl.when(jnp.logical_and(facing(gi, plane), jnp.logical_not(home)))
            def _():
                direct_copy(gi, r).wait_send()

        def sent():
            a2a_copy(r).wait_send()
            for h in range(2):
                q_copy(r, h).wait_send()
            o_copy(r).wait_send()

        if r:
            sent()
        else:
            pl.when(jnp.logical_not(home))(sent)
    for s in range(steps):
        other_copy(s).wait_send()
    for r in range(G):
        o_copy(r).wait_recv()


def body(hidden_states, queries, key_matrix, value_matrix, stretch_table):
    tokens, width = hidden_states.shape
    G = KEY_VALUE_HEADS // lax.axis_size("tp")
    NG = lax.axis_size("ctx") // (2 * G)
    S = tokens // 2
    R = queries.shape[1] // (G * D)
    rows_at = min(ROWS, R * S)
    any_ = pl.BlockSpec(memory_space=pl.ANY)
    bf, f32 = jnp.bfloat16, jnp.float32
    dma = pltpu.SemaphoreType.DMA
    return pl.pallas_call(
        functools.partial(kernel, G, R, NG, S),
        out_shape=jax.ShapeDtypeStruct(queries.shape, bf),
        in_specs=[pl.BlockSpec(memory_space=pltpu.SMEM)] + [any_] * 4,
        out_specs=any_,
        scratch_shapes=[
            pltpu.VMEM((tokens, width), bf),
            pltpu.VMEM((2 * G, width, 2 * D), bf),
            pltpu.VMEM((2 * G, tokens, 2 * D), f32),
            pltpu.VMEM((G, tokens, 2 * D), f32),
            pltpu.VMEM((G, 2, 2, S, D), bf),
            pltpu.VMEM((2, 2, 2 * G * S, D), bf),
            pltpu.VMEM((NG - 1, G // 2, 2, 2, 4 * S, D), bf),
            pltpu.VMEM((G, 2, S, R * D), bf),
            pltpu.VMEM((G, 2, R * S, D), bf),
            pltpu.VMEM((G, 2, R * S, D), f32),
            pltpu.VMEM((G, 2, R * S, D), f32),
            pltpu.VMEM((G, 2, R * S, D), f32),
            pltpu.VMEM((3, rows_at, G * S), f32),
            pltpu.VMEM((2, rows_at, D), f32),
            pltpu.VMEM((3, rows_at, G * S), f32),
            pltpu.VMEM((2, rows_at, D), f32),
            pltpu.VMEM((G, tokens, R * D), bf),
            dma,
            dma((2 * G, 2)),
            dma((G,)),
            dma((G,)),
            dma((G,)),
            dma((2, G)),
            dma((NG - 1, G, 2)),
            dma((G,)),
            dma((NG - 1, G)),
            dma((NG - 1, G)),
            dma((NG - 1, G)),
            dma((G, 2)),
            dma((G, 2)),
            dma((G,)),
            dma((G,)),
        ],
        compiler_params=pltpu.CompilerParams(
            collective_id=0, has_side_effects=True, vmem_limit_bytes=60 * 1024 * 1024
        ),
        name="fused",
    )(stretch_table, hidden_states, queries, key_matrix, value_matrix)


def solution(mesh):
    in_specs = (P("ctx", "tp"), P("ctx", "tp"), P("tp", None), P("tp", None), P())
    out_specs = P("ctx", "tp")
    return jax.shard_map(body, mesh=mesh, in_specs=in_specs, out_specs=out_specs, check_vma=False)
```
